32 devices in a mesh: grp: 2 (over x), seq: 8 (over z, y), head: 2 (over core).
Axes of the slice: x: 2, y: 2, z: 4, core: 2. Of those that a mesh axis runs over, the one named last changes fastest.
Arguments:
- inputs: float32 [4096, 4096], P(('grp', 'seq'), 'head'), parts along dimension 0, may hold values from -6 to 6
- rates: float32 [64, 4096], P('head', ('grp', 'seq')), parts along dimension 1, may hold values from 0.5 to 2
- decay_rate: float32 [64], P('head'), may hold values from 0.00048828125 to 0.03
- skip: float32 [64], P('head'), may hold values from 0.5 to 1.5
- keys_b: float32 [4096, 128], P(('grp', 'seq')), parts along dimension 0, may hold values from -0.5 to 0.5
- keys_c: float32 [4096, 128], P(('grp', 'seq')), parts along dimension 0, may hold values from -0.5 to 0.5
- grad_out: float32 [4096, 4096], P(('grp', 'seq'), 'head'), parts along dimension 0, may hold values from -6 to 6
Outputs:
- output: float32 [4096, 4096], P(('grp', 'seq'), 'head'), parts along dimension 0
- grad_inputs: float32 [4096, 4096], P(('grp', 'seq'), 'head'), parts along dimension 0
- input_key_gradient: float32 [4096, 128], P(('grp', 'seq')), parts along dimension 0
- output_key_gradient: float32 [4096, 128], P(('grp', 'seq')), parts along dimension 0
The draws below stay inside these ranges and needn't reach their ends.
There are 2 independent parts, one for each index of `grp`. The reference program is written for one: setup_inputs(seed, part) draws one part's arguments, and reference() takes and returns one part's arrays. A program takes and returns all parts, laid end to end along the dimension named above; an argument that names none is the same for every part. Nothing has to cross between parts.
All inputs are finite; a program needn't handle non-finite values.
Results may differ from the reference program's by a relative error of at most 0.00016.
Values sent between devices are 32-bit elements; how exact they have to be, the bound alone decides.
A program may use at most 192 MiB of HBM per device.

```python
import math
import jax
import jax.numpy as jnp
from jax import lax

H = 64
P_SIZE = 64
N = 128
SEQ_LEN = 2048


def steps_of(key, extent, shards, least, high):
    loudness, own = 1.0, jax.random.fold_in(key, 6)
    for position, parts in shards:
        steps = jnp.exp(jax.random.uniform(jax.random.fold_in(own, position), (parts,), jnp.float32, least / len(shards), high / len(shards)))
        loudness = loudness * jnp.repeat(steps, extent[position] // parts).reshape([-1 if axis == position else 1 for axis in range(len(extent))])
    return loudness


def bell_draw(own_key, extent, scale, reach, pieces=(), held_as=jnp.bfloat16):
    drawn = jax.random.normal(own_key, extent, jnp.float32) * scale
    if len(pieces) > 0:
        drawn = steps_of(own_key, extent, pieces, -0.22, 0.18) * drawn
    return jnp.clip(drawn, min=-reach, max=reach).astype(held_as)


def setup_inputs(seed: int = 0, part: int = 0) -> dict:
    streams_of = jax.random.split(jax.random.key(seed), 8)
    part_keys = jax.random.split(jax.random.fold_in(streams_of[7], part), 8)
    inputs = bell_draw(part_keys[0], (SEQ_LEN, H * P_SIZE), 1.0, 6.0, ((0, 8), (1, 2)), jnp.float32)
    rates = jnp.clip(jnp.exp(math.log(2.0) - 1.3862944 * jax.random.uniform(part_keys[1], (H, SEQ_LEN), jnp.float32) ** steps_of(part_keys[1], (H, SEQ_LEN), ((0, 2), (1, 8)), -0.2, 0.2)), 0.5, 2.0)
    decay_rate = jnp.clip(jnp.exp(math.log(0.03) - 4.118061 * jax.random.uniform(streams_of[2], (H,), jnp.float32) ** steps_of(streams_of[2], (H,), ((0, 2),), -0.2, 0.2)), 0.00048828125, 0.03)
    skip = jnp.clip(0.5 + 1.0 * jax.random.uniform(streams_of[3], (H,), jnp.float32) ** steps_of(streams_of[3], (H,), ((0, 2),), -0.2, 0.2), 0.5, 1.5)
    keys_b = bell_draw(part_keys[4], (SEQ_LEN, N), N ** -0.5, 0.5, ((0, 8),), jnp.float32)
    keys_c = bell_draw(part_keys[5], (SEQ_LEN, N), N ** -0.5, 0.5, ((0, 8),), jnp.float32)
    grad_out = bell_draw(part_keys[6], (SEQ_LEN, H * P_SIZE), 1.0, 6.0, ((0, 8), (1, 2)), jnp.float32)
    return {"inputs": inputs, "rates": rates, "decay_rate": decay_rate, "skip": skip, "keys_b": keys_b, "keys_c": keys_c, "grad_out": grad_out}


HIGH = lax.Precision.HIGHEST


def reference(inputs, rates, decay_rate, skip, keys_b, keys_c, grad_out):
    length = inputs.shape[0]
    heads = rates.shape[0]
    width = inputs.shape[1] // heads
    state_size = keys_b.shape[1]
    input_rows = inputs.reshape(length, heads, width)
    dys = grad_out.reshape(length, heads, width)
    steps = rates.T
    factors = jnp.exp(-steps * decay_rate[None, :])
    items = (input_rows, steps, factors, keys_b, keys_c, dys)

    def ahead(state, item):
        x, step, factor, key_b, key_c, grad = item
        state = factor[:, None, None] * state + (step[:, None] * x)[:, :, None] * key_b[None, None, :]
        out = jnp.einsum("hpn,n->hp", state, key_c, precision=HIGH) + skip[:, None] * x
        output_key_gradient = jnp.einsum("hpn,hp->n", state, grad, precision=HIGH)
        return state, (out, output_key_gradient)

    start = jnp.zeros((heads, width, state_size), jnp.float32)
    unused, (outs, grads_c) = lax.scan(ahead, start, items)

    def behind(carry, item):
        x, step, factor, key_b, key_c, grad = item
        adjoint_state = grad[:, :, None] * key_c[None, None, :] + carry
        grad_x = step[:, None] * jnp.einsum("hpn,n->hp", adjoint_state, key_b, precision=HIGH) + skip[:, None] * grad
        input_key_gradient = jnp.einsum("hpn,hp->n", adjoint_state, step[:, None] * x, precision=HIGH)
        return factor[:, None, None] * adjoint_state, (grad_x, input_key_gradient)

    unused_two, (grads_x, grads_b) = lax.scan(behind, start, items, reverse=True)
    return (outs.reshape(length, heads * width), grads_x.reshape(length, heads * width), grads_b, grads_c)
```

```python
import functools

import jax
import jax.numpy as jnp
from jax import lax
from jax.experimental import pallas as pl
from jax.experimental.pallas import tpu as pltpu
from jax.sharding import PartitionSpec as P

HIGH = lax.Precision.HIGHEST
MESH = pl.DeviceIdType.MESH
F32, BF16 = jnp.float32, jnp.bfloat16
LANES = 128
COLS = 256
LAG = 2

NN = (((1,), (0,)), ((), ()))
NT = (((1,), (1,)), ((), ()))


def split(a):
    hi = a.astype(BF16)
    return hi, (a - hi.astype(F32)).astype(BF16)


def dot3(a, b, dims=NN):
    def one(l, r):
        return lax.dot_general(l, r, dims, preferred_element_type=F32)

    return one(a[0], b[0]) + one(a[0], b[1]) + one(a[1], b[0])


def kernel(
    n, nh, x_ref, rates_ref, decay_ref, skip_ref, b_ref, c_ref, dy_ref,
    out_ref, gx_ref, db_ref, dc_ref,
    u_ref, v_ref, vxh, vxl, udh, udl, ft, gt, e_in, a_in, dl_ref, sl_ref, m_ref,
    low_ref, part, got, send_f, recv_f, send_b, recv_b, send_h, recv_h,
):
    grp, me, head = lax.axis_index("grp"), lax.axis_index("seq"), lax.axis_index("head")
    tokens, width = x_ref.shape
    heads = rates_ref.shape[0]
    size = width // heads
    steps = width // COLS
    chunks = width // LANES
    per = COLS // LANES
    has_left, has_right = me > 0, me < n - 1
    barrier = pltpu.get_barrier_semaphore()

    @pl.when(has_left)
    def _():
        pl.semaphore_signal(barrier, inc=1, device_id=(grp, me - 1, head), device_id_type=MESH)

    @pl.when(has_right)
    def _():
        pl.semaphore_signal(barrier, inc=1, device_id=(grp, me + 1, head), device_id_type=MESH)

    for k in range(1, nh):
        other = lax.rem(head + k, nh)
        pl.semaphore_signal(barrier, inc=1, device_id=(grp, me, other), device_id_type=MESH)

    rows = lax.broadcasted_iota(jnp.int32, (tokens, tokens), 0)
    cols = lax.broadcasted_iota(jnp.int32, (tokens, tokens), 1)
    lower = jnp.where(rows >= cols, 1.0, 0.0).astype(F32)
    step_t = rates_ref[...].T
    cum = jnp.dot(lower, -(step_t * decay_ref[...]), precision=HIGH, preferred_element_type=F32)
    u = split(jnp.exp(cum))
    v = split(jnp.exp(-cum) * step_t)
    extra = jnp.concatenate(
        [
            jnp.broadcast_to(jnp.exp(cum[tokens - 1 :, :]), (8, heads)),
            jnp.broadcast_to(skip_ref[...], (8, heads)),
        ],
        axis=0,
    )
    extra_hi = extra.astype(BF16)
    extra_mid, extra_lo = split(extra - extra_hi.astype(F32))
    bt = split(b_ref[...].T)
    ct = split(c_ref[...].T)
    b_s, c_s = split(b_ref[...]), split(c_ref[...])
    low = split(jnp.where(rows >= cols, dot3(c_s, b_s, NT), 0.0))
    upp = split(jnp.where(rows <= cols, dot3(b_s, c_s, NT), 0.0))
    low_ref[0], low_ref[1] = low
    low_ref[2], low_ref[3] = upp

    def prepare(k, _):
        at = pl.ds(pl.multiple_of(k * COLS, COLS), COLS)
        lane = lax.broadcasted_iota(jnp.int32, (heads, COLS), 1) + k * COLS
        row = lax.broadcasted_iota(jnp.int32, (heads, COLS), 0)
        spread = jnp.where((lane >= row * size) & (lane < (row + 1) * size), 1.0, 0.0).astype(BF16)

        def wide(*terms):
            return sum(jnp.dot(t, spread, preferred_element_type=F32) for t in terms)

        u_w, v_w, e_w = wide(*u), wide(*v), wide(extra_hi, extra_mid, extra_lo)
        u_ref[:, at] = u_w
        v_ref[:, at] = v_w
        dl_ref[:, at] = e_w[:8]
        sl_ref[:, at] = e_w[8:]
        vx = split(v_w * x_ref[:, at])
        ud = split(u_w * dy_ref[:, at])
        vxh[:, at], vxl[:, at] = vx
        udh[:, at], udl[:, at] = ud
        f = dot3(bt, vx) * e_w[:1]
        g = dot3(ct, ud)
        for i in range(per):
            ft[k * per + i] = f[:, i * LANES : (i + 1) * LANES]
            gt[k * per + i] = g[:, i * LANES : (i + 1) * LANES]
        return 0

    lax.fori_loop(0, steps, prepare, 0)
    m_ref[...] = jnp.zeros_like(m_ref)

    @pl.when(jnp.logical_not(has_left))
    def _():
        e_in[...] = jnp.zeros_like(e_in)

    @pl.when(jnp.logical_not(has_right))
    def _():
        a_in[...] = jnp.zeros_like(a_in)

    peers = has_left.astype(jnp.int32) + has_right.astype(jnp.int32) + nh - 1
    pl.semaphore_wait(barrier, peers)

    def ahead(k):
        return pltpu.make_async_remote_copy(
            src_ref=ft.at[k], dst_ref=e_in.at[k], send_sem=send_f.at[k], recv_sem=recv_f.at[k],
            device_id=(grp, me + 1, head), device_id_type=MESH,
        )

    def behind(k):
        return pltpu.make_async_remote_copy(
            src_ref=gt.at[k], dst_ref=a_in.at[k], send_sem=send_b.at[k], recv_sem=recv_b.at[k],
            device_id=(grp, me - 1, head), device_id_type=MESH,
        )

    def relay(k, copy, before, after, incoming, own):
        @pl.when(before)
        def _():
            copy(k).wait_recv()

            @pl.when(after)
            def _():
                d = dl_ref[:1, pl.ds(pl.multiple_of(k * LANES, LANES), LANES)]
                own[k] = own[k] + d * incoming[k]

        @pl.when(after)
        def _():
            copy(k).start()

    def inner(k):
        at = pl.ds(pl.multiple_of(k * COLS, COLS), COLS)
        vx = vxh[:, at], vxl[:, at]
        ud = udh[:, at], udl[:, at]
        out_ref[:, at] = dot3((low_ref[0], low_ref[1]), vx)
        gx_ref[:, at] = dot3((low_ref[2], low_ref[3]), ud)
        m_ref[...] += dot3(ud, vx, NT)

    def turn(s, _):
        f = s - me * LAG
        b = s - (n - 1 - me) * LAG

        @pl.when((f >= 0) & (f < chunks))
        def _():
            relay(f, ahead, has_left, has_right, e_in, ft)

        @pl.when((b >= 0) & (b < chunks))
        def _():
            relay(b, behind, has_right, has_left, a_in, gt)

        @pl.when(s < steps)
        def _():
            inner(s)

        return 0

    lax.fori_loop(0, max(steps, chunks + (n - 1) * LAG), turn, 0)

    m = jnp.where(rows >= cols, m_ref[...], 0.0)
    part[0] = dot3(split(m.T), c_s)
    part[1] = dot3(split(m), b_s)

    def finish(k, _):
        at = pl.ds(pl.multiple_of(k * COLS, COLS), COLS)
        e = split(jnp.concatenate([e_in[k * per + i] for i in range(per)], axis=1))
        a = split(jnp.concatenate([a_in[k * per + i] for i in range(per)], axis=1) * dl_ref[:1, at])
        skip_w = sl_ref[:1, at]
        out_ref[:, at] = u_ref[:, at] * (out_ref[:, at] + dot3(c_s, e)) + skip_w * x_ref[:, at]
        gx_ref[:, at] = v_ref[:, at] * (gx_ref[:, at] + dot3(b_s, a)) + skip_w * dy_ref[:, at]
        part[0] += dot3((vxh[:, at], vxl[:, at]), a, NT)
        part[1] += dot3((udh[:, at], udl[:, at]), e, NT)
        return 0

    lax.fori_loop(0, steps, finish, 0)

    def across(k):
        return pltpu.make_async_remote_copy(
            src_ref=part, dst_ref=got.at[k - 1], send_sem=send_h.at[k - 1], recv_sem=recv_h.at[k - 1],
            device_id=(grp, me, lax.rem(head + k, nh)), device_id_type=MESH,
        )

    for k in range(1, nh):
        across(k).start()

    def drain(k, _):
        @pl.when(has_right)
        def _():
            ahead(k).wait_send()

        @pl.when(has_left)
        def _():
            behind(k).wait_send()

        return 0

    lax.fori_loop(0, chunks, drain, 0)
    total_b, total_c = part[0], part[1]
    for k in range(1, nh):
        across(k).wait()
        total_b += got[k - 1, 0]
        total_c += got[k - 1, 1]
    db_ref[...] = total_b
    dc_ref[...] = total_c


def body(n, nh, inputs, rates, decay_rate, skip, keys_b, keys_c, grad_out):
    tokens, width = inputs.shape
    heads = rates.shape[0]
    state = keys_b.shape[1]
    chunks = width // LANES
    vmem = pl.BlockSpec(memory_space=pltpu.VMEM)
    dma = pltpu.SemaphoreType.DMA
    others = max(nh - 1, 1)
    return pl.pallas_call(
        functools.partial(kernel, n, nh),
        out_shape=(
            jax.ShapeDtypeStruct((tokens, width), F32),
            jax.ShapeDtypeStruct((tokens, width), F32),
            jax.ShapeDtypeStruct((tokens, state), F32),
            jax.ShapeDtypeStruct((tokens, state), F32),
        ),
        in_specs=[vmem] * 7,
        out_specs=(vmem,) * 4,
        scratch_shapes=[
            pltpu.VMEM((tokens, width), F32),
            pltpu.VMEM((tokens, width), F32),
            pltpu.VMEM((tokens, width), BF16),
            pltpu.VMEM((tokens, width), BF16),
            pltpu.VMEM((tokens, width), BF16),
            pltpu.VMEM((tokens, width), BF16),
            pltpu.VMEM((chunks, state, LANES), F32),
            pltpu.VMEM((chunks, state, LANES), F32),
            pltpu.VMEM((chunks, state, LANES), F32),
            pltpu.VMEM((chunks, state, LANES), F32),
            pltpu.VMEM((8, width), F32),
            pltpu.VMEM((8, width), F32),
            pltpu.VMEM((tokens, tokens), F32),
            pltpu.VMEM((4, tokens, tokens), BF16),
            pltpu.VMEM((2, tokens, state), F32),
            pltpu.VMEM((others, 2, tokens, state), F32),
            dma((chunks,)),
            dma((chunks,)),
            dma((chunks,)),
            dma((chunks,)),
            dma((others,)),
            dma((others,)),
        ],
        compiler_params=pltpu.CompilerParams(collective_id=0, has_side_effects=True),
        name="mixer",
    )(inputs, rates, decay_rate[None, :], skip[None, :], keys_b, keys_c, grad_out)


def solution(mesh):
    in_specs = (
        P(("grp", "seq"), "head"),
        P("head", ("grp", "seq")),
        P("head"),
        P("head"),
        P(("grp", "seq"), None),
        P(("grp", "seq"), None),
        P(("grp", "seq"), "head"),
    )
    out_specs = (
        P(("grp", "seq"), "head"),
        P(("grp", "seq"), "head"),
        P(("grp", "seq"), None),
        P(("grp", "seq"), None),
    )
    run = functools.partial(body, mesh.shape["seq"], mesh.shape["head"])
    return jax.shard_map(run, mesh=mesh, in_specs=in_specs, out_specs=out_specs, check_vma=False)
```

```python
import functools

import jax
import jax.numpy as jnp
from jax import lax
from jax.experimental import pallas as pl
from jax.experimental.pallas import tpu as pltpu
from jax.sharding import PartitionSpec as P

HIGH = lax.Precision.HIGHEST
MESH = pl.DeviceIdType.MESH
F32, BF16 = jnp.float32, jnp.bfloat16
LANES = 128
COLS = 256

NN = (((1,), (0,)), ((), ()))
NT = (((1,), (1,)), ((), ()))


def split(a):
    hi = a.astype(BF16)
    return hi, (a - hi.astype(F32)).astype(BF16)


def dot3(a, b, dims=NN):
    def one(l, r):
        return lax.dot_general(l, r, dims, preferred_element_type=F32)

    return one(a[0], b[0]) + one(a[0], b[1]) + one(a[1], b[0])


def split3(a):
    hi = a.astype(BF16)
    return (hi,) + split(a - hi.astype(F32))


def kernel(
    n, nh, x_ref, rates_ref, decay_ref, skip_ref, b_ref, c_ref, dy_ref,
    out_ref, gx_ref, db_ref, dc_ref,
    u_ref, v_ref, vxh, vxl, udh, udl, near, own, got_near, got_chain, got_back,
    tot_ref, tot_in, dl_ref, sl_ref, pl_ref, m_ref, low_ref, part, got,
    send_n, recv_n, send_c, recv_c, send_j, recv_j, send_h, recv_h, send_t, recv_t,
):
    grp, me, head = lax.axis_index("grp"), lax.axis_index("seq"), lax.axis_index("head")
    tokens, width = x_ref.shape
    heads = rates_ref.shape[0]
    size = width // heads
    steps = width // COLS
    chunks = width // LANES
    per = COLS // LANES
    late = lax.rem(me, 2)
    forward = late == 1
    mate = me + 1 - 2 * late
    stride = 4 * late - 2
    first, last = me < 2, me >= n - 2
    has_in = (forward & jnp.logical_not(first)) | (jnp.logical_not(forward) & jnp.logical_not(last))
    has_out = (forward & jnp.logical_not(last)) | (jnp.logical_not(forward) & jnp.logical_not(first))
    barrier = pltpu.get_barrier_semaphore()

    def greet(seq, core):
        pl.semaphore_signal(barrier, inc=1, device_id=(grp, seq, core), device_id_type=MESH)

    greet(mate, head)

    @pl.when(has_in)
    def _():
        greet(me - stride, head)

    @pl.when(has_out)
    def _():
        greet(me + stride, head)

    for k in range(1, nh):
        greet(me, lax.rem(head + k, nh))

    rows = lax.broadcasted_iota(jnp.int32, (tokens, tokens), 0)
    cols = lax.broadcasted_iota(jnp.int32, (tokens, tokens), 1)
    lower = jnp.where(rows >= cols, 1.0, 0.0).astype(F32)
    step_t = rates_ref[...].T
    cum = jnp.dot(lower, -(step_t * decay_ref[...]), precision=HIGH, preferred_element_type=F32)
    u = split(jnp.exp(cum))
    v = split(jnp.exp(-cum) * step_t)
    tot_ref[...] = jnp.broadcast_to(jnp.exp(cum[tokens - 1 :, :]), (8, heads))
    extra = split3(
        jnp.concatenate([tot_ref[...], jnp.broadcast_to(skip_ref[...], (8, heads))], axis=0)
    )
    b_s, c_s = split(b_ref[...]), split(c_ref[...])
    bt = split(b_ref[...].T)
    ct = split(c_ref[...].T)

    def spread(k):
        lane = lax.broadcasted_iota(jnp.int32, (heads, COLS), 1) + k * COLS
        row = lax.broadcasted_iota(jnp.int32, (heads, COLS), 0)
        return jnp.where((lane >= row * size) & (lane < (row + 1) * size), 1.0, 0.0).astype(BF16)

    def wide(k, terms):
        return sum(jnp.dot(t, spread(k), preferred_element_type=F32) for t in terms)

    def columns(k):
        return pl.ds(pl.multiple_of(k * COLS, COLS), COLS)

    def lanes(k):
        return pl.ds(pl.multiple_of(k * LANES, LANES), LANES)

    def remote(src, dst, sends, recvs, k, to):
        return pltpu.make_async_remote_copy(
            src_ref=src.at[k], dst_ref=dst.at[k], send_sem=sends.at[k], recv_sem=recvs.at[k],
            device_id=(grp, to, head), device_id_type=MESH,
        )

    def to_mate(k):
        return remote(near, got_near, send_n, recv_n, k, mate)

    def onward(k):
        return remote(own, got_chain, send_c, recv_c, k, me + stride)

    def back(k):
        return remote(got_chain, got_back, send_j, recv_j, k, mate)

    total_to_mate = pltpu.make_async_remote_copy(
        src_ref=tot_ref, dst_ref=tot_in, send_sem=send_t.at[0], recv_sem=recv_t.at[0],
        device_id=(grp, mate, head), device_id_type=MESH,
    )
    amount = has_in.astype(jnp.int32) + has_out.astype(jnp.int32) + nh
    pl.semaphore_wait(barrier, amount)
    total_to_mate.start()

    def prepare(k, _):
        at = columns(k)
        u_w, v_w, e_w = wide(k, u), wide(k, v), wide(k, extra)
        u_ref[:, at] = u_w
        v_ref[:, at] = v_w
        dl_ref[:, at] = e_w[:8]
        sl_ref[:, at] = e_w[8:]
        vx = split(v_w * x_ref[:, at])
        ud = split(u_w * dy_ref[:, at])
        vxh[:, at], vxl[:, at] = vx
        udh[:, at], udl[:, at] = ud
        f = dot3(bt, vx) * e_w[:1]
        g = dot3(ct, ud)
        to, keep = jnp.where(forward, g, f), jnp.where(forward, f, g)
        for i in range(per):
            near[k * per + i] = to[:, i * LANES : (i + 1) * LANES]
            own[k * per + i] = keep[:, i * LANES : (i + 1) * LANES]
        for i in range(per):
            to_mate(k * per + i).start()
        return 0

    lax.fori_loop(0, steps, prepare, 0)
    low_ref[0], low_ref[1] = split(jnp.where(rows >= cols, dot3(c_s, b_s, NT), 0.0))
    low_ref[2], low_ref[3] = split(jnp.where(rows <= cols, dot3(b_s, c_s, NT), 0.0))
    m_ref[...] = jnp.zeros_like(m_ref)
    part[...] = jnp.zeros_like(part)
    total_to_mate.wait_recv()
    mates = split3(tot_in[...])

    def inner(k):
        at = columns(k)
        vx = vxh[:, at], vxl[:, at]
        ud = udh[:, at], udl[:, at]
        out_ref[:, at] = dot3((low_ref[0], low_ref[1]), vx)
        gx_ref[:, at] = dot3((low_ref[2], low_ref[3]), ud)
        m_ref[...] += dot3(ud, vx, NT)

    def gather(ref, k):
        return jnp.concatenate([ref[k * per + i] for i in range(per)], axis=1)

    def finish_out(ref, k):
        at = columns(k)
        e = split(gather(ref, k))
        out_ref[:, at] = u_ref[:, at] * (out_ref[:, at] + dot3(c_s, e)) + sl_ref[:1, at] * x_ref[:, at]
        part[1] += dot3((udh[:, at], udl[:, at]), e, NT)

    def finish_gx(ref, k):
        at = columns(k)
        a = split(gather(ref, k) * dl_ref[:1, at])
        gx_ref[:, at] = v_ref[:, at] * (gx_ref[:, at] + dot3(b_s, a)) + sl_ref[:1, at] * dy_ref[:, at]
        part[0] += dot3((vxh[:, at], vxl[:, at]), a, NT)

    def chain(k, _):
        at = columns(k)
        inner(k)
        pl_ref[:, at] = wide(k, mates)
        for i in range(per):
            c = k * per + i
            to_mate(c).wait_recv()

            @pl.when(has_in)
            def _():
                onward(c).wait_recv()
                got_near[c] = got_near[c] + pl_ref[:1, lanes(c)] * got_chain[c]

            @pl.when(has_out)
            def _():
                own[c] = own[c] + dl_ref[:1, lanes(c)] * got_near[c]
                onward(c).start()

            @pl.when(has_in)
            def _():
                back(c).start()

        @pl.when(forward)
        def _():
            finish_out(got_near, k)

        @pl.when(jnp.logical_not(forward))
        def _():
            finish_gx(got_near, k)

        return 0

    lax.fori_loop(0, steps, chain, 0)
    m = jnp.where(rows >= cols, m_ref[...], 0.0)
    part[0] += dot3(split(m.T), c_s)
    part[1] += dot3(split(m), b_s)

    @pl.when(jnp.logical_not(has_out))
    def _():
        got_back[...] = jnp.zeros_like(got_back)

    def close(k, _):
        @pl.when(has_out)
        def _():
            for i in range(per):
                back(k * per + i).wait_recv()

        @pl.when(forward)
        def _():
            finish_gx(got_back, k)

        @pl.when(jnp.logical_not(forward))
        def _():
            finish_out(got_back, k)

        return 0

    lax.fori_loop(0, steps, close, 0)

    def across(k):
        return pltpu.make_async_remote_copy(
            src_ref=part, dst_ref=got.at[k - 1], send_sem=send_h.at[k - 1], recv_sem=recv_h.at[k - 1],
            device_id=(grp, me, lax.rem(head + k, nh)), device_id_type=MESH,
        )

    for k in range(1, nh):
        across(k).start()

    total_to_mate.wait_send()

    def drain(k, _):
        to_mate(k).wait_send()

        @pl.when(has_out)
        def _():
            onward(k).wait_send()

        @pl.when(has_in)
        def _():
            back(k).wait_send()

        return 0

    lax.fori_loop(0, chunks, drain, 0)
    total_b, total_c = part[0], part[1]
    for k in range(1, nh):
        across(k).wait()
        total_b += got[k - 1, 0]
        total_c += got[k - 1, 1]
    db_ref[...] = total_b
    dc_ref[...] = total_c


def body(n, nh, inputs, rates, decay_rate, skip, keys_b, keys_c, grad_out):
    tokens, width = inputs.shape
    heads = rates.shape[0]
    state = keys_b.shape[1]
    chunks = width // LANES
    vmem = pl.BlockSpec(memory_space=pltpu.VMEM)
    dma = pltpu.SemaphoreType.DMA
    others = max(nh - 1, 1)
    return pl.pallas_call(
        functools.partial(kernel, n, nh),
        out_shape=(
            jax.ShapeDtypeStruct((tokens, width), F32),
            jax.ShapeDtypeStruct((tokens, width), F32),
            jax.ShapeDtypeStruct((tokens, state), F32),
            jax.ShapeDtypeStruct((tokens, state), F32),
        ),
        in_specs=[vmem] * 7,
        out_specs=(vmem,) * 4,
        scratch_shapes=[
            pltpu.VMEM((tokens, width), F32),
            pltpu.VMEM((tokens, width), F32),
            pltpu.VMEM((tokens, width), BF16),
            pltpu.VMEM((tokens, width), BF16),
            pltpu.VMEM((tokens, width), BF16),
            pltpu.VMEM((tokens, width), BF16),
            pltpu.VMEM((chunks, state, LANES), F32),
            pltpu.VMEM((chunks, state, LANES), F32),
            pltpu.VMEM((chunks, state, LANES), F32),
            pltpu.VMEM((chunks, state, LANES), F32),
            pltpu.VMEM((chunks, state, LANES), F32),
            pltpu.VMEM((8, heads), F32),
            pltpu.VMEM((8, heads), F32),
            pltpu.VMEM((8, width), F32),
            pltpu.VMEM((8, width), F32),
            pltpu.VMEM((8, width), F32),
            pltpu.VMEM((tokens, tokens), F32),
            pltpu.VMEM((4, tokens, tokens), BF16),
            pltpu.VMEM((2, tokens, state), F32),
            pltpu.VMEM((others, 2, tokens, state), F32),
            dma((chunks,)),
            dma((chunks,)),
            dma((chunks,)),
            dma((chunks,)),
            dma((chunks,)),
            dma((chunks,)),
            dma((others,)),
            dma((others,)),
            dma((1,)),
            dma((1,)),
        ],
        compiler_params=pltpu.CompilerParams(collective_id=0, has_side_effects=True),
        name="mixer",
    )(inputs, rates, decay_rate[None, :], skip[None, :], keys_b, keys_c, grad_out)


def solution(mesh):
    in_specs = (
        P(("grp", "seq"), "head"),
        P("head", ("grp", "seq")),
        P("head"),
        P("head"),
        P(("grp", "seq"), None),
        P(("grp", "seq"), None),
        P(("grp", "seq"), "head"),
    )
    out_specs = (
        P(("grp", "seq"), "head"),
        P(("grp", "seq"), "head"),
        P(("grp", "seq"), None),
        P(("grp", "seq"), None),
    )
    run = functools.partial(body, mesh.shape["seq"], mesh.shape["head"])
    return jax.shard_map(run, mesh=mesh, in_specs=in_specs, out_specs=out_specs, check_vma=False)
```

```python
import functools

import jax
import jax.numpy as jnp
from jax import lax
from jax.experimental import pallas as pl
from jax.experimental.pallas import tpu as pltpu
from jax.sharding import PartitionSpec as P

HIGH = lax.Precision.HIGHEST
MESH = pl.DeviceIdType.MESH
F32, BF16 = jnp.float32, jnp.bfloat16
LANES = 128
VMEM_BYTES = 67043328
COLS = 256

NN = (((1,), (0,)), ((), ()))
NT = (((1,), (1,)), ((), ()))


def split(a):
    hi = a.astype(BF16)
    return hi, (a - hi.astype(F32)).astype(BF16)


def dot3(a, b, dims=NN):
    def one(l, r):
        return lax.dot_general(l, r, dims, preferred_element_type=F32)

    return one(a[0], b[0]) + one(a[0], b[1]) + one(a[1], b[0])


def split3(a):
    hi = a.astype(BF16)
    return (hi,) + split(a - hi.astype(F32))


def kernel(
    n, nh, x_hbm, rates_ref, decay_ref, skip_ref, b_ref, c_ref, dy_hbm,
    out_ref, gx_ref, db_ref, dc_ref,
    x_ref, dy_ref, u_ref, v_ref, vxh, vxl, udh, udl, near, own, got_near, got_chain, got_back,
    tot_ref, tot_in, dl_ref, sl_ref, pl_ref, m_ref, low_ref, part, got,
    send_n, recv_n, send_c, recv_c, send_j, recv_j, send_h, recv_h, send_t, recv_t, load_x, load_dy,
):
    grp, me, head = lax.axis_index("grp"), lax.axis_index("seq"), lax.axis_index("head")
    tokens, width = x_hbm.shape
    heads = rates_ref.shape[0]
    size = width // heads
    steps = width // COLS
    chunks = width // LANES
    per = COLS // LANES

    def load(src, dst, sems, k):
        at = pl.ds(pl.multiple_of(k * COLS, COLS), COLS)
        return pltpu.make_async_copy(src.at[:, at], dst.at[:, at], sems.at[k])

    for k in range(steps):
        load(x_hbm, x_ref, load_x, k).start()
        load(dy_hbm, dy_ref, load_dy, k).start()
    late = lax.rem(me, 2)
    forward = late == 1
    mate = me + 1 - 2 * late
    stride = 4 * late - 2
    first, last = me < 2, me >= n - 2
    has_in = (forward & jnp.logical_not(first)) | (jnp.logical_not(forward) & jnp.logical_not(last))
    has_out = (forward & jnp.logical_not(last)) | (jnp.logical_not(forward) & jnp.logical_not(first))
    barrier = pltpu.get_barrier_semaphore()

    def greet(seq, core):
        pl.semaphore_signal(barrier, inc=1, device_id=(grp, seq, core), device_id_type=MESH)

    greet(mate, head)

    @pl.when(has_in)
    def _():
        greet(me - stride, head)

    @pl.when(has_out)
    def _():
        greet(me + stride, head)

    for k in range(1, nh):
        greet(me, lax.rem(head + k, nh))

    rows = lax.broadcasted_iota(jnp.int32, (tokens, tokens), 0)
    cols = lax.broadcasted_iota(jnp.int32, (tokens, tokens), 1)
    lower = jnp.where(rows >= cols, 1.0, 0.0).astype(F32)
    step_t = rates_ref[...].T
    cum = jnp.dot(lower, -(step_t * decay_ref[...]), precision=HIGH, preferred_element_type=F32)
    u = split(jnp.exp(cum))
    v = split(jnp.exp(-cum) * step_t)
    tot_ref[...] = jnp.broadcast_to(jnp.exp(cum[tokens - 1 :, :]), (8, heads))
    extra = split3(
        jnp.concatenate([tot_ref[...], jnp.broadcast_to(skip_ref[...], (8, heads))], axis=0)
    )
    b_s, c_s = split(b_ref[...]), split(c_ref[...])
    bt = split(b_ref[...].T)
    ct = split(c_ref[...].T)

    def spread(k):
        lane = lax.broadcasted_iota(jnp.int32, (heads, COLS), 1) + k * COLS
        row = lax.broadcasted_iota(jnp.int32, (heads, COLS), 0)
        return jnp.where((lane >= row * size) & (lane < (row + 1) * size), 1.0, 0.0).astype(BF16)

    def wide(k, terms):
        return sum(jnp.dot(t, spread(k), preferred_element_type=F32) for t in terms)

    def columns(k):
        return pl.ds(pl.multiple_of(k * COLS, COLS), COLS)

    def lanes(k):
        return pl.ds(pl.multiple_of(k * LANES, LANES), LANES)

    def remote(src, dst, sends, recvs, k, to):
        return pltpu.make_async_remote_copy(
            src_ref=src.at[k], dst_ref=dst.at[k], send_sem=sends.at[k], recv_sem=recvs.at[k],
            device_id=(grp, to, head), device_id_type=MESH,
        )

    def to_mate(k):
        return remote(near, got_near, send_n, recv_n, k, mate)

    def onward(k):
        return remote(own, got_chain, send_c, recv_c, k, me + stride)

    def back(k):
        return remote(got_chain, got_back, send_j, recv_j, k, mate)

    total_to_mate = pltpu.make_async_remote_copy(
        src_ref=tot_ref, dst_ref=tot_in, send_sem=send_t.at[0], recv_sem=recv_t.at[0],
        device_id=(grp, mate, head), device_id_type=MESH,
    )
    amount = has_in.astype(jnp.int32) + has_out.astype(jnp.int32) + nh
    pl.semaphore_wait(barrier, amount)
    total_to_mate.start()

    def prepare(k, _):
        at = columns(k)
        u_w, v_w, e_w = wide(k, u), wide(k, v), wide(k, extra)
        u_ref[:, at] = u_w
        v_ref[:, at] = v_w
        dl_ref[:, at] = e_w[:8]
        sl_ref[:, at] = e_w[8:]
        load(x_hbm, x_ref, load_x, k).wait()
        load(dy_hbm, dy_ref, load_dy, k).wait()
        vx = split(v_w * x_ref[:, at])
        ud = split(u_w * dy_ref[:, at])
        vxh[:, at], vxl[:, at] = vx
        udh[:, at], udl[:, at] = ud
        f = dot3(bt, vx) * e_w[:1]
        g = dot3(ct, ud)
        to, keep = jnp.where(forward, g, f), jnp.where(forward, f, g)
        for i in range(per):
            near[k * per + i] = to[:, i * LANES : (i + 1) * LANES]
            own[k * per + i] = keep[:, i * LANES : (i + 1) * LANES]
        for i in range(per):
            to_mate(k * per + i).start()
        return 0

    lax.fori_loop(0, steps, prepare, 0)
    low_ref[0], low_ref[1] = split(jnp.where(rows >= cols, dot3(c_s, b_s, NT), 0.0))
    low_ref[2], low_ref[3] = split(jnp.where(rows <= cols, dot3(b_s, c_s, NT), 0.0))
    m_ref[...] = jnp.zeros_like(m_ref)
    part[...] = jnp.zeros_like(part)
    total_to_mate.wait_recv()
    mates = split3(tot_in[...])

    def inner(k):
        at = columns(k)
        vx = vxh[:, at], vxl[:, at]
        ud = udh[:, at], udl[:, at]
        out_ref[:, at] = dot3((low_ref[0], low_ref[1]), vx)
        gx_ref[:, at] = dot3((low_ref[2], low_ref[3]), ud)
        m_ref[...] += dot3(ud, vx, NT)

    def gather(ref, k):
        return jnp.concatenate([ref[k * per + i] for i in range(per)], axis=1)

    def finish_out(ref, k):
        at = columns(k)
        e = split(gather(ref, k))
        out_ref[:, at] = u_ref[:, at] * (out_ref[:, at] + dot3(c_s, e)) + sl_ref[:1, at] * x_ref[:, at]
        part[1] += dot3((udh[:, at], udl[:, at]), e, NT)

    def finish_gx(ref, k):
        at = columns(k)
        a = split(gather(ref, k) * dl_ref[:1, at])
        gx_ref[:, at] = v_ref[:, at] * (gx_ref[:, at] + dot3(b_s, a)) + sl_ref[:1, at] * dy_ref[:, at]
        part[0] += dot3((vxh[:, at], vxl[:, at]), a, NT)

    def chain(k, _):
        at = columns(k)
        inner(k)
        pl_ref[:, at] = wide(k, mates)
        for i in range(per):
            c = k * per + i
            to_mate(c).wait_recv()

            @pl.when(has_in)
            def _():
                onward(c).wait_recv()
                got_near[c] = got_near[c] + pl_ref[:1, lanes(c)] * got_chain[c]

            @pl.when(has_out)
            def _():
                own[c] = own[c] + dl_ref[:1, lanes(c)] * got_near[c]
                onward(c).start()

            @pl.when(has_in)
            def _():
                back(c).start()

        @pl.when(forward)
        def _():
            finish_out(got_near, k)

        @pl.when(jnp.logical_not(forward))
        def _():
            finish_gx(got_near, k)

        return 0

    lax.fori_loop(0, steps, chain, 0)
    m = jnp.where(rows >= cols, m_ref[...], 0.0)
    part[0] += dot3(split(m.T), c_s)
    part[1] += dot3(split(m), b_s)

    def across(k, which):
        return pltpu.make_async_remote_copy(
            src_ref=part.at[which], dst_ref=got.at[k - 1, which],
            send_sem=send_h.at[k - 1, which], recv_sem=recv_h.at[k - 1, which],
            device_id=(grp, me, lax.rem(head + k, nh)), device_id_type=MESH,
        )

    for k in range(1, nh):
        across(k, late).start()

    @pl.when(jnp.logical_not(has_out))
    def _():
        got_back[...] = jnp.zeros_like(got_back)

    def close(k, _):
        @pl.when(has_out)
        def _():
            for i in range(per):
                back(k * per + i).wait_recv()

        @pl.when(forward)
        def _():
            finish_gx(got_back, k)

        @pl.when(jnp.logical_not(forward))
        def _():
            finish_out(got_back, k)

        return 0

    lax.fori_loop(0, steps, close, 0)

    for k in range(1, nh):
        across(k, 1 - late).start()

    total_to_mate.wait_send()

    def drain(k, _):
        to_mate(k).wait_send()

        @pl.when(has_out)
        def _():
            onward(k).wait_send()

        @pl.when(has_in)
        def _():
            back(k).wait_send()

        return 0

    lax.fori_loop(0, chunks, drain, 0)
    total_b, total_c = part[0], part[1]
    for k in range(1, nh):
        across(k, 0).wait()
        across(k, 1).wait()
        total_b += got[k - 1, 0]
        total_c += got[k - 1, 1]
    db_ref[...] = total_b
    dc_ref[...] = total_c


def body(n, nh, inputs, rates, decay_rate, skip, keys_b, keys_c, grad_out):
    tokens, width = inputs.shape
    heads = rates.shape[0]
    state = keys_b.shape[1]
    chunks = width // LANES
    vmem = pl.BlockSpec(memory_space=pltpu.VMEM)
    hbm = pl.BlockSpec(memory_space=pltpu.HBM)
    dma = pltpu.SemaphoreType.DMA
    others = max(nh - 1, 1)
    outputs = 2 * tokens * (width + state) * 4
    limit = VMEM_BYTES - outputs - 2**16
    return pl.pallas_call(
        functools.partial(kernel, n, nh),
        out_shape=(
            pltpu.VMEM((tokens, width), F32),
            pltpu.VMEM((tokens, width), F32),
            pltpu.VMEM((tokens, state), F32),
            pltpu.VMEM((tokens, state), F32),
        ),
        in_specs=[hbm] + [vmem] * 5 + [hbm],
        out_specs=(vmem,) * 4,
        scratch_shapes=[
            pltpu.VMEM((tokens, width), F32),
            pltpu.VMEM((tokens, width), F32),
            pltpu.VMEM((tokens, width), F32),
            pltpu.VMEM((tokens, width), F32),
            pltpu.VMEM((tokens, width), BF16),
            pltpu.VMEM((tokens, width), BF16),
            pltpu.VMEM((tokens, width), BF16),
            pltpu.VMEM((tokens, width), BF16),
            pltpu.VMEM((chunks, state, LANES), F32),
            pltpu.VMEM((chunks, state, LANES), F32),
            pltpu.VMEM((chunks, state, LANES), F32),
            pltpu.VMEM((chunks, state, LANES), F32),
            pltpu.VMEM((chunks, state, LANES), F32),
            pltpu.VMEM((8, heads), F32),
            pltpu.VMEM((8, heads), F32),
            pltpu.VMEM((8, width), F32),
            pltpu.VMEM((8, width), F32),
            pltpu.VMEM((8, width), F32),
            pltpu.VMEM((tokens, tokens), F32),
            pltpu.VMEM((4, tokens, tokens), BF16),
            pltpu.VMEM((2, tokens, state), F32),
            pltpu.VMEM((others, 2, tokens, state), F32),
            dma((chunks,)),
            dma((chunks,)),
            dma((chunks,)),
            dma((chunks,)),
            dma((chunks,)),
            dma((chunks,)),
            dma((others, 2)),
            dma((others, 2)),
            dma((1,)),
            dma((1,)),
            dma((width // COLS,)),
            dma((width // COLS,)),
        ],
        compiler_params=pltpu.CompilerParams(
            collective_id=0, has_side_effects=True, vmem_limit_bytes=limit
        ),
        name="mixer",
    )(inputs, rates, decay_rate[None, :], skip[None, :], keys_b, keys_c, grad_out)


def solution(mesh):
    in_specs = (
        P(("grp", "seq"), "head"),
        P("head", ("grp", "seq")),
        P("head"),
        P("head"),
        P(("grp", "seq"), None),
        P(("grp", "seq"), None),
        P(("grp", "seq"), "head"),
    )
    out_specs = (
        P(("grp", "seq"), "head"),
        P(("grp", "seq"), "head"),
        P(("grp", "seq"), None),
        P(("grp", "seq"), None),
    )
    run = functools.partial(body, mesh.shape["seq"], mesh.shape["head"])
    return jax.shard_map(run, mesh=mesh, in_specs=in_specs, out_specs=out_specs, check_vma=False)
```
